32 devices in a mesh: surf: 8 (over y, x, core), probe: 4 (over z).
Axes of the slice: x: 2, y: 2, z: 4, core: 2. Of those that a mesh axis runs over, the one named last changes fastest.
Arguments:
- probes: bfloat16 [32, 65536], P('probe', 'surf'), may hold values from -6 to 6
- sigma: float32 [65536], P('surf'), may hold values from 0.5 to 2
- prior_patch: bfloat16 [128, 128], replicated, may hold values from -0.5 to 0.5
- owner_map: int32 [1024], P('surf'), may hold values from 0 to 7, as said below
- block_perm: int32 [1024], P('surf'), may hold values from 0 to 127, as said below
- col_counts: int32 [1024], P('surf'), may hold values from 1 to 64
- coef: bfloat16 [1024, 1024], P('surf'), may hold values from 0.5 to 1.5
- obs_weight: bfloat16 [1024, 64], P('surf'), may hold values from 0.25 to 1
- column_op: bfloat16 [1024, 1024], replicated, may hold values from -0.1875 to 0.1875
Outputs:
- hess: float32 [32, 65536], P('probe', 'surf')
- diag_est: float32 [65536], P('surf')
- quad: float32 [32], P('probe')
The draws below stay inside these ranges and needn't reach their ends.
Inputs may be any that keep to these rules, and one draw needn't show every extreme that they name: `owner_map`: the 128 blocks of each surface device go to 8 different column owners, 16 to each. The pairs (owner_map, block_perm) name every slot of every column owner exactly once; a column owner receives 16 blocks from each of 8 surface devices.
All inputs are finite; a program needn't handle non-finite values.
Results may differ from the reference program's by a relative error of at most 0.005.
Values may be sent and summed in bfloat16 or wider, within the bound.
A program may use at most 64 MiB of HBM per device.

```python
import math
import jax
import jax.numpy as jnp
from jax import lax

P_SIZE = 32
BS = 64
PATCH = 128
NBD = 128
CAP = 16
NB = 1024
NS = 65536
VOL = 1024
N_SURF = 8


def owner_and_slot(key):
    groups = NBD // CAP
    key_order = jax.random.fold_in(key, 11)
    key_offset = jax.random.fold_in(key, 12)
    key_blocks = jax.random.fold_in(key, 13)
    key_slots = jax.random.fold_in(key, 14)
    relabel = jax.random.permutation(key_order, N_SURF)
    place = jnp.argsort(relabel)
    offsets = jax.random.permutation(key_offset, N_SURF)[:groups]
    order = jax.vmap(lambda k: jax.random.permutation(k, NBD))(jax.random.split(key_blocks, N_SURF))
    position = jnp.argsort(order, axis=1)
    group = position // CAP
    within = position % CAP
    owner = relabel[(place[:, None] - offsets[group]) % N_SURF]
    slot_tables = jax.vmap(lambda k: jax.random.permutation(k, NBD))(jax.random.split(key_slots, N_SURF))
    slot = slot_tables[owner, group * CAP + within]
    return (owner.reshape(-1).astype(jnp.int32), slot.reshape(-1).astype(jnp.int32))


def draw_owner_map(key, part):
    return owner_and_slot(key)[0]


def draw_block_perm(key, part):
    return owner_and_slot(key)[1]


def place_ends(entries, own_key, low, largest):
    longest = entries.shape.index(max(entries.shape))
    spots = []
    for shift in (0, 1):
        where = [jax.random.randint(jax.random.fold_in(own_key, axis), (), 0, length) for axis, length in enumerate(entries.shape)]
        where[longest] = (where[longest] + shift) % entries.shape[longest]
        spots.append(tuple(where))
    return entries.at[spots[0]].set(low).at[spots[1]].set(largest)


def level_of(key, shape, pieces, least, high):
    def one(dim, parts):
        heights = jax.random.uniform(jax.random.fold_in(jax.random.fold_in(key, 6), dim), (parts,), jnp.float32, least / len(pieces), high / len(pieces))
        return jnp.repeat(jnp.exp(heights), shape[dim] // parts).reshape((-1,) + (1,) * (len(shape) - dim - 1))

    loudness = one(*pieces[0])
    for cut in pieces[1:]:
        loudness = loudness * one(*cut)
    return loudness


def noise(rng, extent, scale, most, cuts=(), kind=jnp.bfloat16):
    values = jax.random.normal(rng, extent, jnp.float32) * scale
    if len(cuts) > 0:
        values = level_of(rng, extent, cuts, -0.22, 0.18) * values
    return jnp.clip(values, min=-most, max=most).astype(kind)


def setup_inputs(seed: int = 0) -> dict:
    arg_keys = jax.random.split(jax.random.key(seed), 10)
    probes = noise(arg_keys[0], (P_SIZE, NS), 1.0, 6.0, ((0, 4), (1, 8)))
    sigma = jnp.clip(jnp.exp(math.log(2.0) - 1.3862944 * jax.random.uniform(arg_keys[1], (NS,), jnp.float32) ** level_of(arg_keys[1], (NS,), ((0, 8),), -0.2, 0.2)), 0.5, 2.0)
    prior_patch = noise(arg_keys[2], (PATCH, PATCH), PATCH ** -0.5, 0.5)
    owner_map = draw_owner_map(jax.random.fold_in(arg_keys[9], 71), 0)
    block_perm = draw_block_perm(jax.random.fold_in(arg_keys[9], 71), 0)
    col_counts = place_ends(jax.random.randint(arg_keys[5], (NB,), 1, BS + 1), jax.random.fold_in(arg_keys[5], 1), 1, BS).astype(jnp.int32)
    coef = jnp.clip(0.5 + 1.0 * jax.random.uniform(arg_keys[6], (NB, VOL), jnp.float32) ** level_of(arg_keys[6], (NB, VOL), ((0, 8),), -0.2, 0.2), 0.5, 1.5).astype(jnp.bfloat16)
    obs_weight = jnp.clip(0.25 + 0.75 * jax.random.uniform(arg_keys[7], (NB, BS), jnp.float32) ** level_of(arg_keys[7], (NB, BS), ((0, 8),), -0.2, 0.2), 0.25, 1.0).astype(jnp.bfloat16)
    column_op = noise(arg_keys[8], (VOL, VOL), VOL ** -0.5, 0.1875)
    return dict(probes=probes, sigma=sigma, prior_patch=prior_patch, owner_map=owner_map, block_perm=block_perm, col_counts=col_counts, coef=coef, obs_weight=obs_weight, column_op=column_op)


def column_term(fields, coef_rows, obs_rows, counts, valid, column_op):
    rows, width, cols = fields.shape
    layers = coef_rows.shape[1] // cols
    column = lax.broadcasted_iota(jnp.int32, (rows, cols), 1)
    keep = jnp.where((column < counts[:, None]) & valid[:, None], 1.0, 0.0).astype(jnp.float32)
    coef_full = coef_rows.astype(jnp.float32).reshape(rows, 1, layers, cols) * keep[:, None, None, :]
    lifted = (fields.astype(jnp.float32)[:, :, None, :] * coef_full).astype(jnp.bfloat16)
    state = jnp.dot(lifted.reshape(rows * width, layers * cols), column_op, preferred_element_type=jnp.float32)
    weighted = (state.reshape(rows, width, layers, cols) * obs_rows.astype(jnp.float32)[:, None, None, :]).astype(jnp.bfloat16)
    adjoint = lax.dot_general(weighted.reshape(rows * width, layers * cols), column_op, (((1,), (1,)), ((), ())), preferred_element_type=jnp.float32)
    return jnp.sum(adjoint.reshape(rows, width, layers, cols) * coef_full, axis=2)


def reference(probes, sigma, prior_patch, owner_map, block_perm, col_counts, coef, obs_weight, column_op):
    grouped = probes.reshape(P_SIZE, NS // PATCH, PATCH).astype(jnp.float32)
    mixed = jnp.einsum("pki,ij->pkj", grouped, prior_patch.astype(jnp.float32))
    spread = (mixed.reshape(P_SIZE, NS) * sigma[None, :]).astype(jnp.bfloat16)
    fields = spread.reshape(P_SIZE, NB, BS).transpose(1, 0, 2)
    target = (owner_map * NBD + block_perm).astype(jnp.int32)
    coef_rows = coef[target]
    obs_rows = obs_weight[target]
    valid = jnp.ones((NBD,), dtype=bool)

    def one_group(items):
        return column_term(items[0], items[1], items[2], items[3], valid, column_op)

    sens = lax.map(one_group, (fields.reshape(N_SURF, NBD, P_SIZE, BS), coef_rows.reshape(N_SURF, NBD, VOL), obs_rows.reshape(N_SURF, NBD, BS), col_counts.reshape(N_SURF, NBD)))
    sens = sens.reshape(NB, P_SIZE, BS).transpose(1, 0, 2).reshape(P_SIZE, NS)
    scaled = (sens * sigma[None, :]).reshape(P_SIZE, NS // PATCH, PATCH)
    back = jnp.einsum("pkj,ij->pki", scaled, prior_patch.astype(jnp.float32), precision=lax.Precision.HIGHEST).reshape(P_SIZE, NS)
    values = probes.astype(jnp.float32)
    hess = values + back
    product = values * back
    diag_est = jnp.sum(product, axis=0) / P_SIZE
    quad = jnp.sum(product, axis=1)
    return hess, diag_est, quad
```

```python
import functools

import jax
import jax.numpy as jnp
from jax import lax
from jax.experimental import pallas as pl
from jax.experimental.pallas import tpu as pltpu
from jax.sharding import PartitionSpec as P

F32 = jnp.float32
BF16 = jnp.bfloat16
NT = (((1,), (1,)), ((), ()))
CHUNKS = 1


def kernel(
    n, z, total_probes,
    owner_hbm, slot_hbm, count_hbm, obs_hbm, patch_hbm, sigma_hbm, probes_hbm, coef_hbm, op_hbm,
    hess_ref, diag_ref, quad_ref,
    owner_ref, slot_ref, count_ref, obs_ref, patch_ref, sigma_ref, probes_ref,
    op_ref, ext_ref, ask_out, ask_in, row_out, row_in, coef_ref, weight_ref, spread_ref, lift_ref, diag_in, quad_in,
    load_sem, ask_send, ask_recv, row_send, row_recv, diag_send, diag_recv, quad_send, quad_recv,
):
    width, nodes = probes_ref.shape
    blocks, vol = coef_hbm.shape
    cols = obs_ref.shape[0]
    patch = patch_ref.shape[0]
    groups = nodes // patch
    depth = blocks // n
    me = lax.axis_index("surf")
    zme = lax.axis_index("probe")
    barrier = pltpu.get_barrier_semaphore()

    def surf_peer(i):
        return lax.rem(me + i, n)

    def probe_peer(i):
        return lax.rem(zme + i, z)

    def greet(i, c):
        pl.semaphore_signal(barrier, inc=1, device_id={"surf": surf_peer(i)}, device_id_type=pl.DeviceIdType.MESH)
        return c

    def greet_z(i, c):
        pl.semaphore_signal(barrier, inc=1, device_id={"probe": probe_peer(i)}, device_id_type=pl.DeviceIdType.MESH)
        return c

    lax.fori_loop(1, n, greet, 0)
    lax.fori_loop(1, z, greet_z, 0)

    smalls = (
        (owner_hbm, owner_ref), (slot_hbm, slot_ref), (count_hbm, count_ref), (obs_hbm, obs_ref),
        (patch_hbm, patch_ref), (sigma_hbm, sigma_ref), (probes_hbm, probes_ref),
    )
    loads = [pltpu.make_async_copy(src, dst, load_sem.at[i]) for i, (src, dst) in enumerate(smalls)]
    load_coef = pltpu.make_async_copy(coef_hbm, ext_ref.at[:, pl.ds(0, vol)], load_sem.at[7])
    load_op = pltpu.make_async_copy(op_hbm, op_ref, load_sem.at[8])
    for load in loads + [load_coef, load_op]:
        load.start()
    for load in loads[:4]:
        load.wait()

    square = (blocks, blocks)
    down = lax.broadcasted_iota(jnp.int32, square, 0)
    across = lax.broadcasted_iota(jnp.int32, square, 1)
    owner = jnp.broadcast_to(owner_ref[...], square).astype(F32)
    same = (owner == jnp.transpose(owner)) & (down < across)
    rank = jnp.sum(jnp.where(same, 1.0, 0.0), axis=0, keepdims=True)
    position = owner * depth + rank
    chosen = position == down.astype(F32)
    slots = jnp.broadcast_to(slot_ref[...], square).astype(F32)
    asked = jnp.sum(jnp.where(chosen, slots, 0.0), axis=1, keepdims=True)
    mine = across == me * depth + lax.rem(down, depth)
    asked = jnp.where(mine, jnp.broadcast_to(asked, square), 0.0).astype(jnp.int32)
    ask_out[...] = jnp.sum(asked.reshape(n, depth, blocks), axis=1, keepdims=True)
    ask_in[pl.ds(me, 1)] = ask_out[pl.ds(me, 1)]
    order = (jnp.transpose(position) == across.astype(F32)).astype(F32).astype(BF16)
    counts = jnp.transpose(jnp.broadcast_to(count_ref[...], square).astype(F32))
    lane = lax.broadcasted_iota(jnp.int32, (blocks, patch), 1)
    keep = jnp.where(lax.rem(lane, cols).astype(F32) < counts, 1.0, 0.0)
    twice = (
        lax.rem(lax.broadcasted_iota(jnp.int32, (cols, patch), 1), cols)
        == lax.broadcasted_iota(jnp.int32, (cols, patch), 0)
    ).astype(F32).astype(BF16)
    ext_ref[:, vol:] = lax.dot_general(
        obs_ref[...], twice, (((0,), (0,)), ((), ())), preferred_element_type=F32
    ).astype(BF16)

    pl.semaphore_wait(barrier, (n - 1) + (z - 1))

    def ask(i):
        return pltpu.make_async_remote_copy(
            src_ref=ask_out.at[surf_peer(i)],
            dst_ref=ask_in.at[me],
            send_sem=ask_send.at[i],
            recv_sem=ask_recv.at[i],
            device_id={"surf": surf_peer(i)},
            device_id_type=pl.DeviceIdType.MESH,
        )

    def row(i):
        return pltpu.make_async_remote_copy(
            src_ref=row_out.at[surf_peer(i)],
            dst_ref=row_in.at[me],
            send_sem=row_send.at[i],
            recv_sem=row_recv.at[i],
            device_id={"surf": surf_peer(i)},
            device_id_type=pl.DeviceIdType.MESH,
        )

    def quad_copy(i):
        return pltpu.make_async_remote_copy(
            src_ref=quad_in.at[me],
            dst_ref=quad_in.at[me],
            send_sem=quad_send.at[i],
            recv_sem=quad_recv.at[i],
            device_id={"surf": surf_peer(i)},
            device_id_type=pl.DeviceIdType.MESH,
        )

    per = groups // CHUNKS

    def diag_copy(c, i):
        part = pl.ds(pl.multiple_of(c * per, per), per)
        return pltpu.make_async_remote_copy(
            src_ref=diag_in.at[zme, part],
            dst_ref=diag_in.at[zme, part],
            send_sem=diag_send.at[c, i],
            recv_sem=diag_recv.at[c, i],
            device_id={"probe": probe_peer(i)},
            device_id_type=pl.DeviceIdType.MESH,
        )

    def each(lo, hi, f):
        def step(i, c):
            f(i)
            return c

        lax.fori_loop(lo, hi, step, 0)

    each(1, n, lambda i: ask(i).start())

    for load in loads[4:]:
        load.wait()
    values = probes_ref[...].astype(F32)
    stacked = jnp.concatenate([values[:, k * patch:(k + 1) * patch] for k in range(groups)], axis=0)
    mixed = jnp.dot(stacked.astype(BF16), patch_ref[...], preferred_element_type=F32)
    for k in range(groups):
        spread_ref[k] = (mixed[k * width:(k + 1) * width] * sigma_ref[k:k + 1, :]).astype(BF16).astype(F32)

    load_coef.wait()
    each(1, n, lambda i: ask(i).wait_recv())
    wanted = jnp.broadcast_to(jnp.sum(ask_in[...], axis=0), square).astype(F32)
    pick = (jnp.transpose(wanted) == across.astype(F32)).astype(F32).astype(BF16)
    rows = jnp.dot(pick, ext_ref[...], preferred_element_type=F32).astype(BF16)
    row_out[...] = rows.reshape(row_out.shape)
    row_in[pl.ds(me, 1)] = row_out[pl.ds(me, 1)]
    each(1, n, lambda i: row(i).start())
    each(1, n, lambda i: ask(i).wait_send())
    load_op.wait()
    each(1, n, lambda i: row(i).wait_recv())
    mine = jnp.dot(order, row_in[...].reshape(blocks, row_in.shape[2]), preferred_element_type=F32)
    for t in range(vol // patch):
        coef_ref[:, t * patch:(t + 1) * patch] = mine[:, t * patch:(t + 1) * patch] * keep
    weight_ref[...] = mine[:, vol:]

    low = lax.broadcasted_iota(jnp.int32, (width, patch), 1) < cols
    tiles = vol // patch

    def chunk(c, energy):
        rows_of = 2 * per
        coef_at = coef_ref[pl.ds(pl.multiple_of(c * rows_of, rows_of), rows_of), :]
        weight_at = weight_ref[pl.ds(pl.multiple_of(c * rows_of, rows_of), rows_of), :]
        sigma_at = sigma_ref[pl.ds(pl.multiple_of(c * per, per), per), :]
        for g in range(per):
            k = c * per + g
            field = spread_ref[k]
            turned = pltpu.roll(field, cols, 1)
            pair = (jnp.where(low, field, turned), jnp.where(low, turned, field))
            for half in range(2):
                spot = slice(2 * g + half, 2 * g + half + 1)
                at = (2 * g + half) * width
                for t in range(tiles):
                    span = slice(t * patch, (t + 1) * patch)
                    lift_ref[at:at + width, span] = pair[half] * coef_at[spot, span]
        state = jnp.dot(lift_ref[...].astype(BF16), op_ref[...], preferred_element_type=F32)
        parts = []
        for g in range(2 * per):
            obs_row = weight_at[g:g + 1, :]
            obs_row = jnp.concatenate([jnp.broadcast_to(obs_row, (width, patch))] * tiles, axis=1)
            parts.append(state[g * width:(g + 1) * width] * obs_row)
        weighted = jnp.concatenate(parts, axis=0).astype(BF16)
        adjoint = lax.dot_general(weighted, op_ref[...], NT, preferred_element_type=F32)
        scaled = []
        for g in range(per):
            folded = []
            for half in range(2):
                at = (2 * g + half) * width
                spot = slice(2 * g + half, 2 * g + half + 1)
                total = None
                for t in range(tiles):
                    span = slice(t * patch, (t + 1) * patch)
                    term = adjoint[at:at + width, span] * coef_at[spot, span]
                    total = term if total is None else total + term
                folded.append(total + pltpu.roll(total, cols, 1))
            scaled.append(jnp.where(low, folded[0], folded[1]) * sigma_at[g:g + 1, :])
        scaled = jnp.concatenate(scaled, axis=0)
        high = scaled.astype(BF16)
        rest = (scaled - high.astype(F32)).astype(BF16)
        back = lax.dot_general(high, patch_ref[...], NT, preferred_element_type=F32) + lax.dot_general(
            rest, patch_ref[...], NT, preferred_element_type=F32
        )
        lines = []
        for g in range(per):
            k = c * per + g
            span = pl.ds(pl.multiple_of(k * patch, patch), patch)
            value = probes_ref[:, span].astype(F32)
            term = back[g * width:(g + 1) * width]
            hess_ref[:, span] = value + term
            product = value * term
            energy = energy + product
            lines.append(jnp.sum(product, axis=0, keepdims=True))
        diag_in[zme, pl.ds(pl.multiple_of(c * per, per), per), :] = jnp.concatenate(lines, axis=0)
        each(1, z, lambda i: diag_copy(c, i).start())
        return energy

    energy = lax.fori_loop(0, CHUNKS, chunk, jnp.zeros((width, patch), F32))
    quad_in[me] = energy
    each(1, n, lambda i: quad_copy(i).start())
    each(1, n, lambda i: row(i).wait_send())
    each(0, CHUNKS, lambda c: each(1, z, lambda i: diag_copy(c, i).wait_recv()))
    total = diag_in[0]
    for i in range(1, z):
        total = total + diag_in[i]
    diag_ref[...] = total * (1.0 / total_probes)
    each(1, n, lambda i: quad_copy(i).wait_recv())
    energy = lax.fori_loop(1, n, lambda i, s: s + quad_in[i], quad_in[0])
    energy = jnp.broadcast_to(jnp.sum(energy, axis=1, keepdims=True), (width, patch))
    diagonal = lax.broadcasted_iota(jnp.int32, (width, patch), 0) == lax.broadcasted_iota(jnp.int32, (width, patch), 1)
    quad_ref[...] = jnp.sum(jnp.where(diagonal, energy, 0.0), axis=0, keepdims=True)[:, :width]
    each(0, CHUNKS, lambda c: each(1, z, lambda i: diag_copy(c, i).wait_send()))
    each(1, n, lambda i: quad_copy(i).wait_send())


def settle(hess_in, diag_in, quad_in, hess_out, diag_out, quad_out, sem):
    stops = ((hess_in, hess_out), (diag_in, diag_out), (quad_in, quad_out))
    store = [pltpu.make_async_copy(src, dst, sem.at[i]) for i, (src, dst) in enumerate(stops)]
    for copy in store:
        copy.start()
    for copy in store:
        copy.wait()


def solution(mesh):
    n, z = mesh.shape["surf"], mesh.shape["probe"]

    def body(probes, sigma, prior_patch, owner_map, block_perm, col_counts, coef, obs_weight, column_op):
        width, nodes = probes.shape
        blocks, vol = coef.shape
        patch = prior_patch.shape[0]
        cols = obs_weight.shape[1]
        groups = nodes // patch
        depth = blocks // n
        vmem = pl.BlockSpec(memory_space=pltpu.VMEM)
        hbm = pl.BlockSpec(memory_space=pl.ANY)
        hess, diag, quad = pl.pallas_call(
            functools.partial(kernel, n, z, width * z),
            out_shape=(
                pltpu.VMEM((width, nodes), F32),
                pltpu.VMEM((groups, patch), F32),
                pltpu.VMEM((1, width), F32),
            ),
            in_specs=[pl.BlockSpec(memory_space=pltpu.HBM)] * 9,
            out_specs=(vmem, vmem, vmem),
            scratch_shapes=[
                pltpu.VMEM((1, blocks), jnp.int32),
                pltpu.VMEM((1, blocks), jnp.int32),
                pltpu.VMEM((1, blocks), jnp.int32),
                pltpu.VMEM((cols, blocks), BF16),
                pltpu.VMEM((patch, patch), BF16),
                pltpu.VMEM((groups, patch), F32),
                pltpu.VMEM((width, nodes), BF16),
                pltpu.VMEM((vol, vol), BF16),
                pltpu.VMEM((blocks, vol + patch), BF16),
                pltpu.VMEM((n, 1, blocks), jnp.int32),
                pltpu.VMEM((n, 1, blocks), jnp.int32),
                pltpu.VMEM((n, depth, vol + patch), BF16),
                pltpu.VMEM((n, depth, vol + patch), BF16),
                pltpu.VMEM((blocks, vol), F32),
                pltpu.VMEM((blocks, patch), F32),
                pltpu.VMEM((groups, width, patch), F32),
                pltpu.VMEM((blocks * width // CHUNKS, vol), F32),
                pltpu.VMEM((z, groups, patch), F32),
                pltpu.VMEM((n, width, patch), F32),
                pltpu.SemaphoreType.DMA((9,)),
                pltpu.SemaphoreType.DMA((n,)),
                pltpu.SemaphoreType.DMA((n,)),
                pltpu.SemaphoreType.DMA((n,)),
                pltpu.SemaphoreType.DMA((n,)),
                pltpu.SemaphoreType.DMA((CHUNKS, z)),
                pltpu.SemaphoreType.DMA((CHUNKS, z)),
                pltpu.SemaphoreType.DMA((n,)),
                pltpu.SemaphoreType.DMA((n,)),
            ],
            compiler_params=pltpu.CompilerParams(collective_id=0, has_side_effects=True, vmem_limit_bytes=32*1024*1024),
        )(*[pltpu.with_memory_space_constraint(x, pltpu.HBM) for x in (
            owner_map.reshape(1, blocks),
            block_perm.reshape(1, blocks),
            col_counts.reshape(1, blocks),
            obs_weight.T,
            prior_patch,
            sigma.reshape(groups, patch),
            probes,
            coef,
            column_op,
        )])
        results = (hess, diag, quad)
        hess, diag, quad = pl.pallas_call(
            settle,
            out_shape=tuple(jax.ShapeDtypeStruct(r.shape, r.dtype) for r in results),
            in_specs=[vmem] * 3,
            out_specs=(hbm,) * 3,
            scratch_shapes=[pltpu.SemaphoreType.DMA((3,))],
            compiler_params=pltpu.CompilerParams(vmem_limit_bytes=1024*1024),
        )(*results)
        return hess, diag.reshape(nodes), quad.reshape(width)

    in_specs = (
        P("probe", "surf"),
        P("surf"),
        P(),
        P("surf"),
        P("surf"),
        P("surf"),
        P("surf", None),
        P("surf", None),
        P(),
    )
    out_specs = (P("probe", "surf"), P("surf"), P("probe"))
    return jax.shard_map(body, mesh=mesh, in_specs=in_specs, out_specs=out_specs, check_vma=False)
```

```python
import functools

import jax
import jax.numpy as jnp
from jax import lax
from jax.experimental import pallas as pl
from jax.experimental.pallas import tpu as pltpu
from jax.sharding import PartitionSpec as P

F32 = jnp.float32
BF16 = jnp.bfloat16
NT = (((1,), (1,)), ((), ()))
PARTS = 4


def kernel(
    n, z, total_probes,
    owner_hbm, slot_hbm, count_hbm, obs_hbm, patch_hbm, sigma_hbm, probes_hbm, coef_hbm, op_hbm,
    hess_ref, diag_ref, quad_ref,
    owner_ref, slot_ref, count_ref, obs_ref, patch_ref, sigma_ref, probes_ref,
    op_ref, ext_ref, ask_out, ask_in, row_out, row_in, value_ref, spread_ref, field_ref, sens_ref, hold_ref,
    diag_in, quad_in,
    load_sem, ask_send, ask_recv, row_send, row_recv, diag_send, diag_recv, quad_send, quad_recv,
):
    width, nodes = probes_ref.shape
    blocks, vol = coef_hbm.shape
    cols = obs_ref.shape[0]
    patch = patch_ref.shape[0]
    groups = nodes // patch
    depth = blocks // n
    tiles = vol // patch
    me = lax.axis_index("surf")
    zme = lax.axis_index("probe")
    barrier = pltpu.get_barrier_semaphore()
    paired = n & (n - 1) == 0

    def flip(i):
        out, bit = 0, 1
        while bit < n:
            out = out + lax.rem(lax.div(me, bit) + lax.div(jnp.int32(i), jnp.int32(bit)), 2) * bit
            bit *= 2
        return out

    def peer_to(i):
        return flip(i) if paired else lax.rem(me + i, n)

    def peer_from(i):
        return flip(i) if paired else lax.rem(me + n - i, n)

    def probe_peer(i):
        return lax.rem(zme + i, z)

    def each(lo, hi, f):
        def step(i, c):
            f(i)
            return c

        lax.fori_loop(lo, hi, step, 0)

    def greet(i):
        pl.semaphore_signal(barrier, inc=1, device_id={"surf": peer_to(n - i)}, device_id_type=pl.DeviceIdType.MESH)

    def greet_z(i):
        pl.semaphore_signal(barrier, inc=1, device_id={"probe": probe_peer(i)}, device_id_type=pl.DeviceIdType.MESH)

    each(1, z, greet_z)
    each(1, n, greet)

    smalls = (
        (owner_hbm, owner_ref), (slot_hbm, slot_ref), (count_hbm, count_ref), (obs_hbm, obs_ref),
        (patch_hbm, patch_ref), (sigma_hbm, sigma_ref), (probes_hbm, probes_ref),
    )
    loads = [pltpu.make_async_copy(src, dst, load_sem.at[i]) for i, (src, dst) in enumerate(smalls)]
    load_coef = pltpu.make_async_copy(coef_hbm, ext_ref.at[:, pl.ds(0, vol)], load_sem.at[7])
    load_op = pltpu.make_async_copy(op_hbm, op_ref, load_sem.at[8])
    for load in loads + [load_coef, load_op]:
        load.start()
    for load in loads[:2]:
        load.wait()

    square = (blocks, blocks)
    down = lax.broadcasted_iota(jnp.int32, square, 0)
    across = lax.broadcasted_iota(jnp.int32, square, 1)
    owner = jnp.broadcast_to(owner_ref[...], square).astype(F32)
    same = (owner == jnp.transpose(owner)) & (down < across)
    rank = jnp.sum(jnp.where(same, 1.0, 0.0), axis=0, keepdims=True)
    key = owner * depth + rank
    turn = lax.div(down, depth)
    if paired:
        turn = jnp.bitwise_xor(turn, me)
    else:
        turn = lax.rem(turn + me, n)
    chosen = key == (turn * depth + lax.rem(down, depth)).astype(F32)
    slots = jnp.broadcast_to(slot_ref[...], square).astype(F32)
    asked = jnp.sum(jnp.where(chosen, slots, 0.0), axis=1, keepdims=True)
    asked = jnp.where(across == down, jnp.broadcast_to(asked, square), 0.0).astype(jnp.int32)
    ask_out[...] = jnp.sum(asked.reshape(n, depth, blocks), axis=1, keepdims=True)

    pl.semaphore_wait(barrier, (n - 1) + (z - 1))

    def ask(i):
        return pltpu.make_async_remote_copy(
            src_ref=ask_out.at[i],
            dst_ref=ask_in.at[i],
            send_sem=ask_send.at[i],
            recv_sem=ask_recv.at[i],
            device_id={"surf": peer_to(i)},
            device_id_type=pl.DeviceIdType.MESH,
        )

    def row(i):
        return pltpu.make_async_remote_copy(
            src_ref=row_out.at[i],
            dst_ref=row_in.at[i],
            send_sem=row_send.at[i],
            recv_sem=row_recv.at[i],
            device_id={"surf": peer_from(i)},
            device_id_type=pl.DeviceIdType.MESH,
        )

    def quad_copy(i):
        return pltpu.make_async_remote_copy(
            src_ref=quad_in.at[me],
            dst_ref=quad_in.at[me],
            send_sem=quad_send.at[i],
            recv_sem=quad_recv.at[i],
            device_id={"surf": peer_to(i)},
            device_id_type=pl.DeviceIdType.MESH,
        )

    def diag_copy(i):
        return pltpu.make_async_remote_copy(
            src_ref=diag_in.at[zme],
            dst_ref=diag_in.at[zme],
            send_sem=diag_send.at[i],
            recv_sem=diag_recv.at[i],
            device_id={"probe": probe_peer(i)},
            device_id_type=pl.DeviceIdType.MESH,
        )

    each(1, n, lambda i: ask(n - i).start())

    for load in loads[2:4]:
        load.wait()
    lane = lax.rem(across, patch)
    block = jnp.sum(jnp.where(chosen, across.astype(F32), 0.0), axis=1, keepdims=True)
    spot = (2 * lax.rem(across, groups) + lax.div(across, groups)).astype(F32)
    place = jnp.where(jnp.broadcast_to(block, square) == spot, 1.0, 0.0)
    gather = place.astype(BF16)
    scatter = jnp.transpose(place).astype(BF16)
    counts = jnp.broadcast_to(count_ref[...], square).astype(F32)
    counts = jnp.sum(jnp.where(chosen, counts, 0.0), axis=1, keepdims=True)
    keep_lane = lax.rem(lax.broadcasted_iota(jnp.int32, (blocks, patch), 1), cols).astype(F32)
    keep = jnp.where(keep_lane < counts, 1.0, 0.0)
    twice = (
        lax.rem(lax.broadcasted_iota(jnp.int32, (cols, patch), 1), cols)
        == lax.broadcasted_iota(jnp.int32, (cols, patch), 0)
    ).astype(F32).astype(BF16)
    ext_ref[:, vol:] = lax.dot_general(
        obs_ref[...], twice, (((0,), (0,)), ((), ())), preferred_element_type=F32
    ).astype(BF16)

    for load in loads[4:]:
        load.wait()
    values = probes_ref[...].astype(F32)
    stacked = jnp.concatenate([values[:, k * patch:(k + 1) * patch] for k in range(groups)], axis=0)
    value_ref[...] = stacked
    mixed = jnp.dot(stacked.astype(BF16), patch_ref[...], preferred_element_type=F32)
    for k in range(groups):
        spread_ref[k * width:(k + 1) * width, :] = (
            (mixed[k * width:(k + 1) * width] * sigma_ref[k:k + 1, :]).astype(BF16).astype(F32)
        )
    low = lax.broadcasted_iota(jnp.int32, (groups, patch), 1) < cols
    halves = []
    for p in range(width):
        field = spread_ref[pl.ds(p, groups, stride=width), :]
        turned = pltpu.roll(field, cols, 1)
        halves.append(jnp.concatenate([jnp.where(low, field, turned), jnp.where(low, turned, field)], axis=0).astype(BF16))
    ordered = jnp.dot(gather, jnp.concatenate(halves, axis=1), preferred_element_type=F32)
    for p in range(width):
        field_ref[p] = (ordered[:, p * patch:(p + 1) * patch] * keep).astype(BF16)

    load_coef.wait()

    def serve(lo, hi):
        each(max(lo, 1), hi, lambda i: ask(i).wait_recv())
        rows_of = (hi - lo) * depth
        shape = (rows_of, blocks)
        wanted = jnp.sum(ask_in[lo:hi], axis=0)
        if lo == 0:
            wanted = wanted + ask_out[0]
        here = lax.broadcasted_iota(jnp.int32, shape, 1)
        diagonal = here == lax.broadcasted_iota(jnp.int32, shape, 0) + lo * depth
        wanted = jnp.sum(jnp.where(diagonal, jnp.broadcast_to(wanted, shape).astype(F32), 0.0), axis=1, keepdims=True)
        pick = jnp.where(jnp.broadcast_to(wanted, shape) == here.astype(F32), 1.0, 0.0).astype(BF16)
        rows = jnp.dot(pick, ext_ref[...], preferred_element_type=F32).astype(BF16)
        row_out[lo:hi] = rows.reshape(hi - lo, depth, rows.shape[1])
        if lo == 0:
            row_in[0] = row_out[0]
        each(max(lo, 1), hi, lambda i: row(i).start())

    step = n // PARTS
    ask_in[0] = jnp.zeros(ask_in.shape[1:], jnp.int32)
    serve(0, step)
    serve(step, (PARTS - 1) * step)
    serve((PARTS - 1) * step, n)
    load_op.wait()

    rows_of = blocks // PARTS
    for g in range(PARTS):
        each(max(g * step, 1), (g + 1) * step, lambda i: row(i).wait_recv())
        span = slice(g * rows_of, (g + 1) * rows_of)
        got = row_in[g * step:(g + 1) * step].reshape(rows_of, row_in.shape[2])
        coef = got[:, :vol]
        weight = got[:, vol:].astype(F32)
        lifted = jnp.concatenate(
            [jnp.concatenate([field_ref[p, span, :]] * tiles, axis=1) * coef for p in range(width)], axis=0
        )
        state = jnp.dot(lifted, op_ref[...], preferred_element_type=F32)
        weight = jnp.concatenate([weight] * tiles, axis=1)
        weighted = jnp.concatenate(
            [(state[p * rows_of:(p + 1) * rows_of] * weight).astype(BF16) for p in range(width)], axis=0
        )
        adjoint = lax.dot_general(weighted, op_ref[...], NT, preferred_element_type=F32)
        coef = coef.astype(F32)
        for p in range(width):
            at = slice(p * rows_of, (p + 1) * rows_of)
            total = None
            for t in range(tiles):
                cut = slice(t * patch, (t + 1) * patch)
                term = adjoint[at, cut] * coef[:, cut]
                total = term if total is None else total + term
            total = (total + pltpu.roll(total, cols, 1)) * keep[span]
            sens_ref[span, p * patch:(p + 1) * patch] = total.astype(BF16)

    split = jnp.dot(scatter, sens_ref[...], preferred_element_type=F32)
    scaled = []
    for p in range(width):
        cut = slice(p * patch, (p + 1) * patch)
        scaled.append((jnp.where(low, split[:groups, cut], split[groups:, cut]) * sigma_ref[...]).astype(BF16))
    back = lax.dot_general(jnp.concatenate(scaled, axis=0), patch_ref[...], NT, preferred_element_type=F32)
    total = None
    energy = []
    for p in range(width):
        term = back[p * groups:(p + 1) * groups]
        value = value_ref[pl.ds(p, groups, stride=width), :]
        product = value * term
        total = product if total is None else total + product
        energy.append(jnp.sum(product, axis=0, keepdims=True))
        hold_ref[pl.ds(p, groups, stride=width), :] = value + term
    diag_in[zme] = total.astype(BF16)
    each(1, z, lambda i: diag_copy(i).start())
    quad_in[me] = jnp.concatenate(energy, axis=0)
    each(1, n, lambda i: quad_copy(n - i).start())
    for k in range(groups):
        hess_ref[:, k * patch:(k + 1) * patch] = hold_ref[k * width:(k + 1) * width, :]
    each(1, n, lambda i: ask(i).wait_send())
    each(1, n, lambda i: row(i).wait_send())
    each(1, n, lambda i: quad_copy(i).wait_recv())
    energy = lax.fori_loop(1, n, lambda i, s: s + quad_in[i], quad_in[0])
    energy = jnp.broadcast_to(jnp.sum(energy, axis=1, keepdims=True), (width, patch))
    diagonal = lax.broadcasted_iota(jnp.int32, (width, patch), 0) == lax.broadcasted_iota(jnp.int32, (width, patch), 1)
    quad_ref[...] = jnp.sum(jnp.where(diagonal, energy, 0.0), axis=0, keepdims=True)[:, :width]
    each(1, n, lambda i: quad_copy(i).wait_send())
    each(1, z, lambda i: diag_copy(i).wait_send())
    each(1, z, lambda i: diag_copy(i).wait_recv())
    total = diag_in[0].astype(F32)
    for i in range(1, z):
        total = total + diag_in[i].astype(F32)
    diag_ref[...] = total * (1.0 / total_probes)


def settle(hess_in, diag_in, quad_in, hess_out, diag_out, quad_out, sem):
    stops = ((hess_in, hess_out), (diag_in, diag_out), (quad_in, quad_out))
    store = [pltpu.make_async_copy(src, dst, sem.at[i]) for i, (src, dst) in enumerate(stops)]
    for copy in store:
        copy.start()
    for copy in store:
        copy.wait()


def solution(mesh):
    n, z = mesh.shape["surf"], mesh.shape["probe"]

    def body(probes, sigma, prior_patch, owner_map, block_perm, col_counts, coef, obs_weight, column_op):
        width, nodes = probes.shape
        blocks, vol = coef.shape
        patch = prior_patch.shape[0]
        cols = obs_weight.shape[1]
        groups = nodes // patch
        depth = blocks // n
        vmem = pl.BlockSpec(memory_space=pltpu.VMEM)
        hbm = pl.BlockSpec(memory_space=pl.ANY)
        operands = (
            owner_map.reshape(1, blocks),
            block_perm.reshape(1, blocks),
            col_counts.reshape(1, blocks),
            obs_weight.T,
            prior_patch,
            sigma.reshape(groups, patch),
            probes,
            coef,
            column_op,
        )
        results = pl.pallas_call(
            functools.partial(kernel, n, z, width * z),
            out_shape=(
                pltpu.VMEM((width, nodes), F32),
                pltpu.VMEM((groups, patch), F32),
                pltpu.VMEM((1, width), F32),
            ),
            in_specs=[pl.BlockSpec(memory_space=pltpu.HBM)] * 9,
            out_specs=(vmem, vmem, vmem),
            scratch_shapes=[
                pltpu.VMEM((1, blocks), jnp.int32),
                pltpu.VMEM((1, blocks), jnp.int32),
                pltpu.VMEM((1, blocks), jnp.int32),
                pltpu.VMEM((cols, blocks), BF16),
                pltpu.VMEM((patch, patch), BF16),
                pltpu.VMEM((groups, patch), F32),
                pltpu.VMEM((width, nodes), BF16),
                pltpu.VMEM((vol, vol), BF16),
                pltpu.VMEM((blocks, vol + patch), BF16),
                pltpu.VMEM((n, 1, blocks), jnp.int32),
                pltpu.VMEM((n, 1, blocks), jnp.int32),
                pltpu.VMEM((n, depth, vol + patch), BF16),
                pltpu.VMEM((n, depth, vol + patch), BF16),
                pltpu.VMEM((groups * width, patch), F32),
                pltpu.VMEM((groups * width, patch), F32),
                pltpu.VMEM((width, blocks, patch), BF16),
                pltpu.VMEM((blocks, width * patch), BF16),
                pltpu.VMEM((groups * width, patch), F32),
                pltpu.VMEM((z, groups, patch), BF16),
                pltpu.VMEM((n, width, patch), F32),
                pltpu.SemaphoreType.DMA((9,)),
                pltpu.SemaphoreType.DMA((n,)),
                pltpu.SemaphoreType.DMA((n,)),
                pltpu.SemaphoreType.DMA((n,)),
                pltpu.SemaphoreType.DMA((n,)),
                pltpu.SemaphoreType.DMA((z,)),
                pltpu.SemaphoreType.DMA((z,)),
                pltpu.SemaphoreType.DMA((n,)),
                pltpu.SemaphoreType.DMA((n,)),
            ],
            compiler_params=pltpu.CompilerParams(
                collective_id=0, has_side_effects=True, vmem_limit_bytes=32 * 1024 * 1024
            ),
        )(*[pltpu.with_memory_space_constraint(x, pltpu.HBM) for x in operands])
        hess, diag, quad = pl.pallas_call(
            settle,
            out_shape=tuple(jax.ShapeDtypeStruct(r.shape, r.dtype) for r in results),
            in_specs=[vmem] * 3,
            out_specs=(hbm,) * 3,
            scratch_shapes=[pltpu.SemaphoreType.DMA((3,))],
            compiler_params=pltpu.CompilerParams(vmem_limit_bytes=1024 * 1024),
        )(*results)
        return hess, diag.reshape(nodes), quad.reshape(width)

    in_specs = (
        P("probe", "surf"),
        P("surf"),
        P(),
        P("surf"),
        P("surf"),
        P("surf"),
        P("surf", None),
        P("surf", None),
        P(),
    )
    out_specs = (P("probe", "surf"), P("surf"), P("probe"))
    return jax.shard_map(body, mesh=mesh, in_specs=in_specs, out_specs=out_specs, check_vma=False)
```

```python
import functools

import jax
import jax.numpy as jnp
from jax import lax
from jax.experimental import pallas as pl
from jax.experimental.pallas import tpu as pltpu
from jax.sharding import PartitionSpec as P

F32 = jnp.float32
BF16 = jnp.bfloat16
NT = (((1,), (1,)), ((), ()))
PARTS = 4
CHUNKS = ((0, 1), (1, 2), (2, 4))


def kernel(
    n, z, total_probes,
    owner_hbm, slot_hbm, count_hbm, obs_hbm, patch_hbm, sigma_hbm, probes_hbm, coef_hbm, op_hbm,
    hess_ref, diag_ref, quad_ref,
    index_ref, obs_ref, patch_ref, sigma_ref, probes_ref,
    op_ref, ext_ref, ask_out, ask_in, row_out, row_in, value_ref, spread_ref, field_ref, sens_ref, hold_ref,
    diag_in, quad_in,
    load_sem, ask_send, ask_recv, row_send, row_recv, diag_send, diag_recv, quad_send, quad_recv,
    answer,
):
    width, nodes = probes_ref.shape
    blocks, vol = coef_hbm.shape
    cols = obs_ref.shape[0]
    patch = patch_ref.shape[0]
    groups = nodes // patch
    depth = blocks // n
    tiles = vol // patch
    me = lax.axis_index("surf")
    zme = lax.axis_index("probe")
    barrier = pltpu.get_barrier_semaphore()
    paired = n & (n - 1) == 0

    signs = []
    if paired:
        bit = 1
        while bit < n:
            signs.append((1 - 2 * lax.rem(lax.div(me, bit), 2)) * bit)
            bit *= 2

    def code(i):
        return (0, 1, 2, 4, 3, 5, 6, 7)[i] if n == 8 else i

    def flip(i):
        out = me
        if isinstance(i, int):
            for b, sign in enumerate(signs):
                if code(i) >> b & 1:
                    out = out + sign
        else:
            for b, sign in enumerate(signs):
                out = out + sign * lax.rem(lax.div(i, jnp.int32(1 << b)), 2)
        return out

    def peer_to(i):
        return flip(i) if paired else lax.rem(me + i, n)

    def peer_from(i):
        return flip(i) if paired else lax.rem(me + n - i, n)

    def probe_peer(i):
        return lax.rem(zme + i, z)

    def each(lo, hi, f):
        if hi - lo <= 8:
            for i in range(lo, hi):
                f(i)
        else:
            lax.fori_loop(lo, hi, lambda i, c: (f(i), c)[1], 0)

    def greet(i):
        pl.semaphore_signal(barrier, inc=1, device_id={"surf": peer_to(n - i)}, device_id_type=pl.DeviceIdType.MESH)

    def tell(sem, lo, hi):
        def step(i, c):
            pl.semaphore_signal(sem, inc=1, device_id={"probe": i}, device_id_type=pl.DeviceIdType.MESH)
            return c

        lax.fori_loop(lo, hi, step, 0)

    def settled(ref, sem):
        pltpu.make_async_copy(ref, ref, sem).wait()

    for i, src in enumerate((owner_hbm, slot_hbm)):
        pltpu.make_async_copy(src, index_ref.at[i], load_sem.at[0]).start()
    each(1, n, greet)
    tell(barrier, zme + 1, z)

    smalls = ((count_hbm, index_ref.at[2]), (obs_hbm, obs_ref), (patch_hbm, patch_ref), (sigma_hbm, sigma_ref), (probes_hbm, probes_ref))
    loads = [pltpu.make_async_copy(src, dst, load_sem.at[1 + i]) for i, (src, dst) in enumerate(smalls)]
    load_coef = pltpu.make_async_copy(coef_hbm, ext_ref.at[:, pl.ds(0, vol)], load_sem.at[6])
    load_op = pltpu.make_async_copy(op_hbm, op_ref, load_sem.at[7])
    for load in loads + [load_coef, load_op]:
        load.start()
    settled(index_ref.at[0:2], load_sem.at[0])

    square = (blocks, blocks)
    down = lax.broadcasted_iota(jnp.int32, square, 0)
    across = lax.broadcasted_iota(jnp.int32, square, 1)
    owner = jnp.broadcast_to(index_ref[0], square).astype(F32)
    same = (owner == jnp.transpose(owner)) & (down < across)
    rank = jnp.sum(jnp.where(same, 1.0, 0.0), axis=0, keepdims=True)
    key = owner * depth + rank
    turn = lax.div(down, depth)
    if n == 8:
        turn = jnp.where(turn == 3, 4, jnp.where(turn == 4, 3, turn))
    if paired:
        turn = jnp.bitwise_xor(turn, me)
    else:
        turn = lax.rem(turn + me, n)
    chosen = key == (turn * depth + lax.rem(down, depth)).astype(F32)
    slots = jnp.broadcast_to(index_ref[1], square).astype(F32)
    asked = jnp.sum(jnp.where(chosen, slots, 0.0), axis=1, keepdims=True)
    asked = jnp.where(across == down, jnp.broadcast_to(asked, square), 0.0).astype(jnp.int32)
    ask_out[...] = jnp.sum(asked.reshape(n, depth, blocks), axis=1, keepdims=True)

    pl.semaphore_wait(barrier, (n - 1) + zme)

    def ask(i, part):
        return pltpu.make_async_remote_copy(
            src_ref=ask_out.at[i],
            dst_ref=ask_in.at[i],
            send_sem=ask_send,
            recv_sem=ask_recv.at[part],
            device_id={"surf": peer_to(i)},
            device_id_type=pl.DeviceIdType.MESH,
        )

    def row(i, part):
        return pltpu.make_async_remote_copy(
            src_ref=row_out.at[i],
            dst_ref=row_in.at[i],
            send_sem=row_send,
            recv_sem=row_recv.at[part],
            device_id={"surf": peer_from(i)},
            device_id_type=pl.DeviceIdType.MESH,
        )

    def quad_copy(i):
        return pltpu.make_async_remote_copy(
            src_ref=quad_in.at[me],
            dst_ref=quad_in.at[me],
            send_sem=quad_send,
            recv_sem=quad_recv,
            device_id={"surf": peer_to(i)},
            device_id_type=pl.DeviceIdType.MESH,
        )

    def diag_copy(i):
        return pltpu.make_async_remote_copy(
            src_ref=diag_in.at[zme],
            dst_ref=diag_in.at[zme],
            send_sem=diag_send,
            recv_sem=diag_recv,
            device_id={"probe": probe_peer(i)},
            device_id_type=pl.DeviceIdType.MESH,
        )

    step = n // PARTS
    for part in reversed(range(PARTS)):
        each(max(part * step, 1), (part + 1) * step, lambda i: ask(i, part).start())
    tell(answer, 0, zme)

    for load in loads[:2]:
        load.wait()
    lane = lax.rem(across, patch)
    block = jnp.sum(jnp.where(chosen, across.astype(F32), 0.0), axis=1, keepdims=True)
    spot = (2 * lax.rem(across, groups) + lax.div(across, groups)).astype(F32)
    place = jnp.where(jnp.broadcast_to(block, square) == spot, 1.0, 0.0)
    gather = place.astype(BF16)
    scatter = jnp.transpose(place).astype(BF16)
    counts = jnp.broadcast_to(index_ref[2], square).astype(F32)
    counts = jnp.sum(jnp.where(chosen, counts, 0.0), axis=1, keepdims=True)
    keep_lane = lax.rem(lax.broadcasted_iota(jnp.int32, (blocks, patch), 1), cols).astype(F32)
    keep = jnp.where(keep_lane < counts, 1.0, 0.0)
    twice = (
        lax.rem(lax.broadcasted_iota(jnp.int32, (cols, patch), 1), cols)
        == lax.broadcasted_iota(jnp.int32, (cols, patch), 0)
    ).astype(F32).astype(BF16)
    ext_ref[:, vol:] = lax.dot_general(
        obs_ref[...], twice, (((0,), (0,)), ((), ())), preferred_element_type=F32
    ).astype(BF16)

    for load in loads[2:]:
        load.wait()
    values = probes_ref[...].astype(F32)
    stacked = jnp.concatenate([values[:, k * patch:(k + 1) * patch] for k in range(groups)], axis=0)
    value_ref[...] = stacked
    mixed = jnp.dot(stacked.astype(BF16), patch_ref[...], preferred_element_type=F32)
    for k in range(groups):
        spread_ref[k * width:(k + 1) * width, :] = (
            (mixed[k * width:(k + 1) * width] * sigma_ref[k:k + 1, :]).astype(BF16).astype(F32)
        )
    low = lax.broadcasted_iota(jnp.int32, (groups, patch), 1) < cols
    halves = []
    for p in range(width):
        field = spread_ref[pl.ds(p, groups, stride=width), :]
        turned = pltpu.roll(field, cols, 1)
        halves.append(jnp.concatenate([jnp.where(low, field, turned), jnp.where(low, turned, field)], axis=0).astype(BF16))
    ordered = jnp.dot(gather, jnp.concatenate(halves, axis=1), preferred_element_type=F32)
    for p in range(width):
        field_ref[p] = (ordered[:, p * patch:(p + 1) * patch] * keep).astype(BF16)

    load_coef.wait()

    def serve(part):
        lo, hi = part * step, (part + 1) * step
        if hi > max(lo, 1):
            settled(ask_in.at[max(lo, 1):hi], ask_recv.at[part])
        rows_of = (hi - lo) * depth
        shape = (rows_of, blocks)
        wanted = jnp.sum(ask_in[lo:hi], axis=0)
        if lo == 0:
            wanted = wanted + ask_out[0]
        here = lax.broadcasted_iota(jnp.int32, shape, 1)
        diagonal = here == lax.broadcasted_iota(jnp.int32, shape, 0) + lo * depth
        wanted = jnp.sum(jnp.where(diagonal, jnp.broadcast_to(wanted, shape).astype(F32), 0.0), axis=1, keepdims=True)
        pick = jnp.where(jnp.broadcast_to(wanted, shape) == here.astype(F32), 1.0, 0.0).astype(BF16)
        rows = jnp.dot(pick, ext_ref[...], preferred_element_type=F32).astype(BF16)
        row_out[lo:hi] = rows.reshape(hi - lo, depth, rows.shape[1])
        if lo == 0:
            row_in[0] = row_out[0]
        each(max(lo, 1), hi, lambda i: row(i, part).start())

    ask_in[0] = jnp.zeros(ask_in.shape[1:], jnp.int32)
    for part in range(PARTS):
        serve(part)
    load_op.wait()

    for first, last in CHUNKS:
        if last == PARTS:

            @pl.when(zme < z - 1)
            def _():
                pl.semaphore_wait(answer, z - 1 - zme)

        for part in range(first, last):
            if (part + 1) * step > max(part * step, 1):
                settled(row_in.at[max(part * step, 1):(part + 1) * step], row_recv.at[part])
        rows_of = (last - first) * step * depth
        span = slice(first * step * depth, last * step * depth)
        got = row_in[first * step:last * step].reshape(rows_of, row_in.shape[2])
        coef = got[:, :vol]
        weight = got[:, vol:].astype(F32)
        lifted = jnp.concatenate(
            [jnp.concatenate([field_ref[p, span, :]] * tiles, axis=1) * coef for p in range(width)], axis=0
        )
        state = jnp.dot(lifted, op_ref[...], preferred_element_type=F32)
        weight = jnp.concatenate([weight] * tiles, axis=1)
        weighted = jnp.concatenate(
            [(state[p * rows_of:(p + 1) * rows_of] * weight).astype(BF16) for p in range(width)], axis=0
        )
        adjoint = lax.dot_general(weighted, op_ref[...], NT, preferred_element_type=F32)
        coef = coef.astype(F32)
        for p in range(width):
            at = slice(p * rows_of, (p + 1) * rows_of)
            total = None
            for t in range(tiles):
                cut = slice(t * patch, (t + 1) * patch)
                term = adjoint[at, cut] * coef[:, cut]
                total = term if total is None else total + term
            total = (total + pltpu.roll(total, cols, 1)) * keep[span]
            sens_ref[span, p * patch:(p + 1) * patch] = total.astype(BF16)

    split = jnp.dot(scatter, sens_ref[...], preferred_element_type=F32)
    scaled = []
    for p in range(width):
        cut = slice(p * patch, (p + 1) * patch)
        scaled.append((jnp.where(low, split[:groups, cut], split[groups:, cut]) * sigma_ref[...]).astype(BF16))
    back = lax.dot_general(jnp.concatenate(scaled, axis=0), patch_ref[...], NT, preferred_element_type=F32)
    total = None
    for p in range(width):
        product = value_ref[pl.ds(p, groups, stride=width), :] * back[p * groups:(p + 1) * groups]
        total = product if total is None else total + product
    diag_in[zme] = total.astype(BF16)
    each(1, z, lambda i: diag_copy(i).start())
    energy = []
    for p in range(width):
        term = back[p * groups:(p + 1) * groups]
        value = value_ref[pl.ds(p, groups, stride=width), :]
        energy.append(jnp.sum(value * term, axis=0, keepdims=True))
        hold_ref[pl.ds(p, groups, stride=width), :] = value + term
    quad_in[me] = jnp.concatenate(energy, axis=0)
    each(1, n, lambda i: quad_copy(n - i).start())
    for k in range(groups):
        hess_ref[:, k * patch:(k + 1) * patch] = hold_ref[k * width:(k + 1) * width, :]
    settled(ask_out.at[1:n], ask_send)
    settled(row_out.at[1:n], row_send)
    settled(quad_in.at[1:n], quad_recv)
    energy = lax.fori_loop(1, n, lambda i, s: s + quad_in[i], quad_in[0])
    energy = jnp.broadcast_to(jnp.sum(energy, axis=1, keepdims=True), (width, patch))
    diagonal = lax.broadcasted_iota(jnp.int32, (width, patch), 0) == lax.broadcasted_iota(jnp.int32, (width, patch), 1)
    quad_ref[...] = jnp.sum(jnp.where(diagonal, energy, 0.0), axis=0, keepdims=True)[:, :width]
    settled(quad_in.at[1:n], quad_send)
    settled(diag_in.at[1:z], diag_send)
    settled(diag_in.at[1:z], diag_recv)
    total = diag_in[0].astype(F32)
    for i in range(1, z):
        total = total + diag_in[i].astype(F32)
    diag_ref[...] = total * (1.0 / total_probes)


def settle(hess_in, diag_in, quad_in, hess_out, diag_out, quad_out, sem):
    stops = ((hess_in, hess_out), (diag_in, diag_out), (quad_in, quad_out))
    store = [pltpu.make_async_copy(src, dst, sem.at[i]) for i, (src, dst) in enumerate(stops)]
    for copy in store:
        copy.start()
    for copy in store:
        copy.wait()


def solution(mesh):
    n, z = mesh.shape["surf"], mesh.shape["probe"]

    def body(probes, sigma, prior_patch, owner_map, block_perm, col_counts, coef, obs_weight, column_op):
        width, nodes = probes.shape
        blocks, vol = coef.shape
        patch = prior_patch.shape[0]
        cols = obs_weight.shape[1]
        groups = nodes // patch
        depth = blocks // n
        vmem = pl.BlockSpec(memory_space=pltpu.VMEM)
        hbm = pl.BlockSpec(memory_space=pl.ANY)
        operands = (
            owner_map.reshape(1, blocks),
            block_perm.reshape(1, blocks),
            col_counts.reshape(1, blocks),
            obs_weight.T,
            prior_patch,
            sigma.reshape(groups, patch),
            probes,
            coef,
            column_op,
        )
        results = pl.pallas_call(
            functools.partial(kernel, n, z, width * z),
            out_shape=(
                pltpu.VMEM((width, nodes), F32),
                pltpu.VMEM((groups, patch), F32),
                pltpu.VMEM((1, width), F32),
            ),
            in_specs=[pl.BlockSpec(memory_space=pltpu.HBM)] * 9,
            out_specs=(vmem, vmem, vmem),
            scratch_shapes=[
                pltpu.VMEM((3, 1, blocks), jnp.int32),
                pltpu.VMEM((cols, blocks), BF16),
                pltpu.VMEM((patch, patch), BF16),
                pltpu.VMEM((groups, patch), F32),
                pltpu.VMEM((width, nodes), BF16),
                pltpu.VMEM((vol, vol), BF16),
                pltpu.VMEM((blocks, vol + patch), BF16),
                pltpu.VMEM((n, 1, blocks), jnp.int32),
                pltpu.VMEM((n, 1, blocks), jnp.int32),
                pltpu.VMEM((n, depth, vol + patch), BF16),
                pltpu.VMEM((n, depth, vol + patch), BF16),
                pltpu.VMEM((groups * width, patch), F32),
                pltpu.VMEM((groups * width, patch), F32),
                pltpu.VMEM((width, blocks, patch), BF16),
                pltpu.VMEM((blocks, width * patch), BF16),
                pltpu.VMEM((groups * width, patch), F32),
                pltpu.VMEM((z, groups, patch), BF16),
                pltpu.VMEM((n, width, patch), F32),
                pltpu.SemaphoreType.DMA((8,)),
                pltpu.SemaphoreType.DMA,
                pltpu.SemaphoreType.DMA((PARTS,)),
                pltpu.SemaphoreType.DMA,
                pltpu.SemaphoreType.DMA((PARTS,)),
                pltpu.SemaphoreType.DMA,
                pltpu.SemaphoreType.DMA,
                pltpu.SemaphoreType.DMA,
                pltpu.SemaphoreType.DMA,
                pltpu.SemaphoreType.REGULAR,
            ],
            compiler_params=pltpu.CompilerParams(
                collective_id=0, has_side_effects=True, vmem_limit_bytes=32 * 1024 * 1024
            ),
        )(*[pltpu.with_memory_space_constraint(x, pltpu.HBM) for x in operands])
        hess, diag, quad = pl.pallas_call(
            settle,
            out_shape=tuple(jax.ShapeDtypeStruct(r.shape, r.dtype) for r in results),
            in_specs=[vmem] * 3,
            out_specs=(hbm,) * 3,
            scratch_shapes=[pltpu.SemaphoreType.DMA((3,))],
            compiler_params=pltpu.CompilerParams(vmem_limit_bytes=1024 * 1024),
        )(*results)
        return hess, diag.reshape(nodes), quad.reshape(width)

    in_specs = (
        P("probe", "surf"),
        P("surf"),
        P(),
        P("surf"),
        P("surf"),
        P("surf"),
        P("surf", None),
        P("surf", None),
        P(),
    )
    out_specs = (P("probe", "surf"), P("surf"), P("probe"))
    return jax.shard_map(body, mesh=mesh, in_specs=in_specs, out_specs=out_specs, check_vma=False)
```

```python
import functools

import jax
import jax.numpy as jnp
from jax import lax
from jax.experimental import pallas as pl
from jax.experimental.pallas import tpu as pltpu
from jax.sharding import PartitionSpec as P

F32 = jnp.float32
BF16 = jnp.bfloat16
NT = (((1,), (1,)), ((), ()))
PARTS = 4
ORDER = (0, 1, 3, 5, 2, 4, 6, 7)


def kernel(
    n, z, total_probes,
    owner_hbm, slot_hbm, count_hbm, obs_hbm, patch_hbm, sigma_hbm, probes_hbm, coef_hbm, op_hbm,
    hess_ref, diag_ref, quad_ref,
    index_ref, obs_ref, patch_ref, sigma_ref, probes_ref,
    op_ref, ext_ref, ask_out, ask_in, row_out, row_in, keep_ref, value_ref, spread_ref, field_ref, sens_ref, hold_ref,
    diag_in, quad_in,
    load_sem, ask_send, ask_recv, row_send, row_recv, diag_send, diag_recv, quad_send, quad_recv,
    answer, relay,
):
    width, nodes = probes_ref.shape
    blocks, vol = coef_hbm.shape
    cols = obs_ref.shape[0]
    patch = patch_ref.shape[0]
    groups = nodes // patch
    depth = blocks // n
    tiles = vol // patch
    me = lax.axis_index("surf")
    zme = lax.axis_index("probe")
    barrier = pltpu.get_barrier_semaphore()
    paired = n & (n - 1) == 0

    signs = []
    if paired:
        bit = 1
        while bit < n:
            signs.append((1 - 2 * lax.rem(lax.div(me, bit), 2)) * bit)
            bit *= 2

    def code(i):
        return ORDER[i] if n == len(ORDER) else i

    def flip(i):
        out = me
        if isinstance(i, int):
            for b, sign in enumerate(signs):
                if code(i) >> b & 1:
                    out = out + sign
        else:
            for b, sign in enumerate(signs):
                bits = lax.rem(lax.div(i, jnp.int32(1 << b)), 2)
                if n == len(ORDER):
                    bits = sum(jnp.where(i == k, code(k) >> b & 1, 0) for k in range(n))
                out = out + sign * bits
        return out

    def peer_to(i):
        return flip(i) if paired else lax.rem(me + i, n)

    def peer_from(i):
        return flip(i) if paired else lax.rem(me + n - i, n)

    def probe_peer(i):
        return lax.rem(zme + i, z)

    def each(lo, hi, f):
        if hi - lo <= 8:
            for i in range(lo, hi):
                f(i)
        else:
            lax.fori_loop(lo, hi, lambda i, c: (f(i), c)[1], 0)

    def greet(i):
        pl.semaphore_signal(barrier, inc=1, device_id={"surf": peer_to(n - i)}, device_id_type=pl.DeviceIdType.MESH)

    def tell(sem, lo, hi):
        def step(i, c):
            pl.semaphore_signal(sem, inc=1, device_id={"probe": i}, device_id_type=pl.DeviceIdType.MESH)
            return c

        lax.fori_loop(lo, hi, step, 0)

    def settled(ref, sem):
        pltpu.make_async_copy(ref, ref, sem).wait()

    for i, src in enumerate((owner_hbm, slot_hbm)):
        pltpu.make_async_copy(src, index_ref.at[i], load_sem.at[0]).start()
    far = n - 2 if n == len(ORDER) else n
    upper = lax.div(me, 4) if n == len(ORDER) else 1
    each(1, far, lambda i: greet(n - i))
    if far < n:

        @pl.when(upper == 0)
        def _():
            each(far, n, lambda i: greet(n - i))

    tell(barrier, zme + 1, z)

    smalls = ((count_hbm, index_ref.at[2]), (obs_hbm, obs_ref), (patch_hbm, patch_ref), (sigma_hbm, sigma_ref), (probes_hbm, probes_ref))
    loads = [pltpu.make_async_copy(src, dst, load_sem.at[1 + i]) for i, (src, dst) in enumerate(smalls)]
    load_coef = pltpu.make_async_copy(coef_hbm, ext_ref.at[:, pl.ds(0, vol)], load_sem.at[6])
    load_op = pltpu.make_async_copy(op_hbm, op_ref, load_sem.at[7])
    for load in loads + [load_coef, load_op]:
        load.start()
    settled(index_ref.at[0:2], load_sem.at[0])

    square = (blocks, blocks)
    down = lax.broadcasted_iota(jnp.int32, square, 0)
    across = lax.broadcasted_iota(jnp.int32, square, 1)
    owner = jnp.broadcast_to(index_ref[0], square).astype(F32)
    same = (owner == jnp.transpose(owner)) & (down < across)
    rank = jnp.sum(jnp.where(same, 1.0, 0.0), axis=0, keepdims=True)
    key = owner * depth + rank
    turn = lax.div(down, depth)
    if n == len(ORDER):
        slot = turn
        for i in range(n):
            turn = jnp.where(slot == i, code(i), turn)
    if paired:
        turn = jnp.bitwise_xor(turn, me)
    else:
        turn = lax.rem(turn + me, n)
    chosen = key == (turn * depth + lax.rem(down, depth)).astype(F32)
    slots = jnp.broadcast_to(index_ref[1], square).astype(F32)
    asked = jnp.sum(jnp.where(chosen, slots, 0.0), axis=1, keepdims=True)
    asked = jnp.where(across == down, jnp.broadcast_to(asked, square), 0.0).astype(jnp.int32)
    ask_out[...] = jnp.sum(asked.reshape(n, depth, blocks), axis=1, keepdims=True)

    pl.semaphore_wait(barrier, (far - 1) + (n - far) * upper + zme)

    def ask(i, part):
        return pltpu.make_async_remote_copy(
            src_ref=ask_out.at[i],
            dst_ref=ask_in.at[i],
            send_sem=ask_send,
            recv_sem=ask_recv.at[part],
            device_id={"surf": peer_to(i)},
            device_id_type=pl.DeviceIdType.MESH,
        )

    def row(i, part):
        return pltpu.make_async_remote_copy(
            src_ref=row_out.at[i],
            dst_ref=row_in.at[i],
            send_sem=row_send,
            recv_sem=row_recv.at[part],
            device_id={"surf": peer_from(i)},
            device_id_type=pl.DeviceIdType.MESH,
        )

    def quad_copy(i):
        return pltpu.make_async_remote_copy(
            src_ref=quad_in.at[me],
            dst_ref=quad_in.at[me],
            send_sem=quad_send,
            recv_sem=quad_recv,
            device_id={"surf": peer_to(i)},
            device_id_type=pl.DeviceIdType.MESH,
        )

    def diag_copy(i):
        return pltpu.make_async_remote_copy(
            src_ref=diag_in.at[zme],
            dst_ref=diag_in.at[zme],
            send_sem=diag_send,
            recv_sem=diag_recv,
            device_id={"probe": probe_peer(i)},
            device_id_type=pl.DeviceIdType.MESH,
        )

    step = n // PARTS

    def ask_far():
        each(far, n, lambda i: ask(i, i // step).start())

    each(1, far, lambda i: ask(i, i // step if isinstance(i, int) else lax.div(i, step)).start())
    if far < n:

        @pl.when(upper == 1)
        def _():
            ask_far()

        @pl.when((upper == 0) & (lax.rem(me, 2) == 1))
        def _():
            for i in (2, 4):
                pl.semaphore_signal(relay, inc=1, device_id={"surf": peer_to(i)}, device_id_type=pl.DeviceIdType.MESH)

    tell(answer, 0, zme)

    for load in loads[:2]:
        load.wait()
    lane = lax.rem(across, patch)
    block = jnp.sum(jnp.where(chosen, across.astype(F32), 0.0), axis=1, keepdims=True)
    spot = (2 * lax.rem(across, groups) + lax.div(across, groups)).astype(F32)
    place = jnp.where(jnp.broadcast_to(block, square) == spot, 1.0, 0.0)
    gather = place.astype(BF16)
    scatter = jnp.transpose(place).astype(BF16)
    counts = jnp.broadcast_to(index_ref[2], square).astype(F32)
    counts = jnp.sum(jnp.where(chosen, counts, 0.0), axis=1, keepdims=True)
    keep_lane = lax.rem(lax.broadcasted_iota(jnp.int32, (blocks, patch), 1), cols).astype(F32)
    keep = jnp.where(keep_lane < counts, 1.0, 0.0)
    keep_ref[...] = keep
    twice = (
        lax.rem(lax.broadcasted_iota(jnp.int32, (cols, patch), 1), cols)
        == lax.broadcasted_iota(jnp.int32, (cols, patch), 0)
    ).astype(F32).astype(BF16)
    ext_ref[:, vol:] = lax.dot_general(
        obs_ref[...], twice, (((0,), (0,)), ((), ())), preferred_element_type=F32
    ).astype(BF16)

    for load in loads[2:]:
        load.wait()
    values = probes_ref[...].astype(F32)
    stacked = jnp.concatenate([values[:, k * patch:(k + 1) * patch] for k in range(groups)], axis=0)
    value_ref[...] = stacked
    mixed = jnp.dot(stacked.astype(BF16), patch_ref[...], preferred_element_type=F32)
    for k in range(groups):
        spread_ref[k * width:(k + 1) * width, :] = (
            (mixed[k * width:(k + 1) * width] * sigma_ref[k:k + 1, :]).astype(BF16).astype(F32)
        )
    low = lax.broadcasted_iota(jnp.int32, (groups, patch), 1) < cols
    halves = []
    for p in range(width):
        field = spread_ref[pl.ds(p, groups, stride=width), :]
        turned = pltpu.roll(field, cols, 1)
        halves.append(jnp.concatenate([jnp.where(low, field, turned), jnp.where(low, turned, field)], axis=0).astype(BF16))
    ordered = jnp.dot(gather, jnp.concatenate(halves, axis=1), preferred_element_type=F32)
    for p in range(width):
        field_ref[p] = (ordered[:, p * patch:(p + 1) * patch] * keep).astype(BF16)

    load_coef.wait()

    ways = (0, 1 + lax.rem(me, 2), 2 - lax.rem(me, 2), 3)
    extent = step * depth

    def arrived(ref, sem, part):
        if isinstance(part, int):
            if (part + 1) * step > max(part * step, 1):
                settled(ref.at[max(part * step, 1):(part + 1) * step], sem.at[part])
        else:
            settled(ref.at[pl.ds(part * step, step)], sem.at[part])

    def start_of(part):
        return part * extent if isinstance(part, int) else pl.multiple_of(part * extent, extent)

    def serve(part):
        arrived(ask_in, ask_recv, part)
        shape = (extent, blocks)
        wanted = jnp.sum(ask_in[pl.ds(part * step, step)], axis=0)
        if isinstance(part, int) and part == 0:
            wanted = wanted + ask_out[0]
        here = lax.broadcasted_iota(jnp.int32, shape, 1)
        diagonal = here == lax.broadcasted_iota(jnp.int32, shape, 0) + part * extent
        wanted = jnp.sum(jnp.where(diagonal, jnp.broadcast_to(wanted, shape).astype(F32), 0.0), axis=1, keepdims=True)
        pick = jnp.where(jnp.broadcast_to(wanted, shape) == here.astype(F32), 1.0, 0.0).astype(BF16)
        rows = jnp.dot(pick, ext_ref[...], preferred_element_type=F32).astype(BF16)
        row_out[pl.ds(part * step, step)] = rows.reshape(step, depth, rows.shape[1])
        if isinstance(part, int) and part == 0:
            row_in[0] = row_out[0]
            each(1, step, lambda i: row(i, part).start())
        elif isinstance(part, int):
            each(part * step, (part + 1) * step, lambda i: row(i, part).start())
        else:
            each(0, step, lambda i: row(part * step + i, part).start())

    ask_in[0] = jnp.zeros(ask_in.shape[1:], jnp.int32)
    for part in ways:
        serve(part)
        if far < n and isinstance(part, int) and part == 0:

            @pl.when(upper == 0)
            def _():
                pl.semaphore_wait(relay, 1)
                ask_far()

    load_op.wait()

    def column(part):
        got = row_in[pl.ds(part * step, step)].reshape(extent, row_in.shape[2])
        coef = got[:, :vol]
        weight = got[:, vol:].astype(F32)
        lifted = jnp.concatenate(
            [jnp.concatenate([field_ref[p, pl.ds(start_of(part), extent), :]] * tiles, axis=1) * coef for p in range(width)],
            axis=0,
        )
        weight = jnp.concatenate([weight] * tiles, axis=1)
        state = jnp.dot(lifted, op_ref[...], preferred_element_type=F32)
        weighted = jnp.concatenate(
            [(state[p * extent:(p + 1) * extent] * weight).astype(BF16) for p in range(width)], axis=0
        )
        adjoint = lax.dot_general(weighted, op_ref[...], NT, preferred_element_type=F32)
        return adjoint

    def fold(part, adjoint):
        coef = row_in[pl.ds(part * step, step)].reshape(extent, row_in.shape[2])[:, :vol].astype(F32)
        span = pl.ds(start_of(part), extent)
        keep = keep_ref[span, :]
        for p in range(width):
            at = slice(p * extent, (p + 1) * extent)
            total = None
            for t in range(tiles):
                cut = slice(t * patch, (t + 1) * patch)
                term = adjoint[at, cut] * coef[:, cut]
                total = term if total is None else total + term
            total = (total + pltpu.roll(total, cols, 1)) * keep
            sens_ref[span, p * patch:(p + 1) * patch] = total.astype(BF16)

    before = None
    for part in ways:
        arrived(row_in, row_recv, part)
        if isinstance(part, int) and part == PARTS - 1:

            @pl.when(zme < z - 1)
            def _():
                pl.semaphore_wait(answer, z - 1 - zme)

        if before is not None:
            fold(*before)
        before = part, column(part)
    fold(*before)

    split = jnp.dot(scatter, sens_ref[...], preferred_element_type=F32)
    scaled = []
    for p in range(width):
        cut = slice(p * patch, (p + 1) * patch)
        scaled.append((jnp.where(low, split[:groups, cut], split[groups:, cut]) * sigma_ref[...]).astype(BF16))
    back = lax.dot_general(jnp.concatenate(scaled, axis=0), patch_ref[...], NT, preferred_element_type=F32)
    total = None
    for p in range(width):
        product = value_ref[pl.ds(p, groups, stride=width), :] * back[p * groups:(p + 1) * groups]
        total = product if total is None else total + product
    diag_in[zme] = total.astype(BF16)
    each(1, z, lambda i: diag_copy(i).start())
    energy = []
    for p in range(width):
        term = back[p * groups:(p + 1) * groups]
        value = value_ref[pl.ds(p, groups, stride=width), :]
        energy.append(jnp.sum(value * term, axis=0, keepdims=True))
        hold_ref[pl.ds(p, groups, stride=width), :] = value + term
    quad_in[me] = jnp.concatenate(energy, axis=0)
    each(1, n, lambda i: quad_copy(n - i).start())
    for k in range(groups):
        hess_ref[:, k * patch:(k + 1) * patch] = hold_ref[k * width:(k + 1) * width, :]
    settled(ask_out.at[1:n], ask_send)
    settled(row_out.at[1:n], row_send)
    settled(quad_in.at[1:n], quad_recv)
    energy = lax.fori_loop(1, n, lambda i, s: s + quad_in[i], quad_in[0])
    energy = jnp.broadcast_to(jnp.sum(energy, axis=1, keepdims=True), (width, patch))
    diagonal = lax.broadcasted_iota(jnp.int32, (width, patch), 0) == lax.broadcasted_iota(jnp.int32, (width, patch), 1)
    quad_ref[...] = jnp.sum(jnp.where(diagonal, energy, 0.0), axis=0, keepdims=True)[:, :width]
    settled(quad_in.at[1:n], quad_send)
    settled(diag_in.at[1:z], diag_send)
    settled(diag_in.at[1:z], diag_recv)
    total = diag_in[0].astype(F32)
    for i in range(1, z):
        total = total + diag_in[i].astype(F32)
    diag_ref[...] = total * (1.0 / total_probes)


def settle(hess_in, diag_in, quad_in, hess_out, diag_out, quad_out, sem):
    stops = ((hess_in, hess_out), (diag_in, diag_out), (quad_in, quad_out))
    store = [pltpu.make_async_copy(src, dst, sem.at[i]) for i, (src, dst) in enumerate(stops)]
    for copy in store:
        copy.start()
    for copy in store:
        copy.wait()


def solution(mesh):
    n, z = mesh.shape["surf"], mesh.shape["probe"]

    def body(probes, sigma, prior_patch, owner_map, block_perm, col_counts, coef, obs_weight, column_op):
        width, nodes = probes.shape
        blocks, vol = coef.shape
        patch = prior_patch.shape[0]
        cols = obs_weight.shape[1]
        groups = nodes // patch
        depth = blocks // n
        vmem = pl.BlockSpec(memory_space=pltpu.VMEM)
        hbm = pl.BlockSpec(memory_space=pl.ANY)
        operands = (
            owner_map.reshape(1, blocks),
            block_perm.reshape(1, blocks),
            col_counts.reshape(1, blocks),
            obs_weight.T,
            prior_patch,
            sigma.reshape(groups, patch),
            probes,
            coef,
            column_op,
        )
        results = pl.pallas_call(
            functools.partial(kernel, n, z, width * z),
            out_shape=(
                pltpu.VMEM((width, nodes), F32),
                pltpu.VMEM((groups, patch), F32),
                pltpu.VMEM((1, width), F32),
            ),
            in_specs=[pl.BlockSpec(memory_space=pltpu.HBM)] * 9,
            out_specs=(vmem, vmem, vmem),
            scratch_shapes=[
                pltpu.VMEM((3, 1, blocks), jnp.int32),
                pltpu.VMEM((cols, blocks), BF16),
                pltpu.VMEM((patch, patch), BF16),
                pltpu.VMEM((groups, patch), F32),
                pltpu.VMEM((width, nodes), BF16),
                pltpu.VMEM((vol, vol), BF16),
                pltpu.VMEM((blocks, vol + patch), BF16),
                pltpu.VMEM((n, 1, blocks), jnp.int32),
                pltpu.VMEM((n, 1, blocks), jnp.int32),
                pltpu.VMEM((n, depth, vol + patch), BF16),
                pltpu.VMEM((n, depth, vol + patch), BF16),
                pltpu.VMEM((blocks, patch), F32),
                pltpu.VMEM((groups * width, patch), F32),
                pltpu.VMEM((groups * width, patch), F32),
                pltpu.VMEM((width, blocks, patch), BF16),
                pltpu.VMEM((blocks, width * patch), BF16),
                pltpu.VMEM((groups * width, patch), F32),
                pltpu.VMEM((z, groups, patch), BF16),
                pltpu.VMEM((n, width, patch), F32),
                pltpu.SemaphoreType.DMA((8,)),
                pltpu.SemaphoreType.DMA,
                pltpu.SemaphoreType.DMA((PARTS,)),
                pltpu.SemaphoreType.DMA,
                pltpu.SemaphoreType.DMA((PARTS,)),
                pltpu.SemaphoreType.DMA,
                pltpu.SemaphoreType.DMA,
                pltpu.SemaphoreType.DMA,
                pltpu.SemaphoreType.DMA,
                pltpu.SemaphoreType.REGULAR,
                pltpu.SemaphoreType.REGULAR,
            ],
            compiler_params=pltpu.CompilerParams(
                collective_id=0, has_side_effects=True, vmem_limit_bytes=32 * 1024 * 1024
            ),
        )(*[pltpu.with_memory_space_constraint(x, pltpu.HBM) for x in operands])
        hess, diag, quad = pl.pallas_call(
            settle,
            out_shape=tuple(jax.ShapeDtypeStruct(r.shape, r.dtype) for r in results),
            in_specs=[vmem] * 3,
            out_specs=(hbm,) * 3,
            scratch_shapes=[pltpu.SemaphoreType.DMA((3,))],
            compiler_params=pltpu.CompilerParams(vmem_limit_bytes=1024 * 1024),
        )(*results)
        return hess, diag.reshape(nodes), quad.reshape(width)

    in_specs = (
        P("probe", "surf"),
        P("surf"),
        P(),
        P("surf"),
        P("surf"),
        P("surf"),
        P("surf", None),
        P("surf", None),
        P(),
    )
    out_specs = (P("probe", "surf"), P("surf"), P("probe"))
    return jax.shard_map(body, mesh=mesh, in_specs=in_specs, out_specs=out_specs, check_vma=False)
```

```python
import functools

import jax
import jax.numpy as jnp
from jax import lax
from jax.experimental import pallas as pl
from jax.experimental.pallas import tpu as pltpu
from jax.sharding import PartitionSpec as P

F32 = jnp.float32
BF16 = jnp.bfloat16
NT = (((1,), (1,)), ((), ()))
PARTS = 4
ORDER = (0, 1, 3, 5, 2, 4, 6, 7)


def kernel(
    n, z, total_probes,
    owner_hbm, slot_hbm, count_hbm, obs_hbm, patch_hbm, sigma_hbm, probes_hbm, coef_hbm, op_hbm,
    hess_ref, diag_ref, quad_ref,
    index_ref, obs_ref, patch_ref, sigma_ref, probes_ref,
    op_ref, ext_ref, ask_out, ask_in, row_out, row_in, keep_ref, value_ref, spread_ref, field_ref, sens_ref, hold_ref,
    diag_in, quad_in,
    load_sem, ask_send, ask_recv, row_send, row_recv, diag_send, diag_recv, quad_send, quad_recv,
    answer, relay,
):
    width, nodes = probes_ref.shape
    blocks, vol = coef_hbm.shape
    cols = obs_ref.shape[0]
    patch = patch_ref.shape[0]
    groups = nodes // patch
    depth = blocks // n
    tiles = vol // patch
    me = lax.axis_index("surf")
    zme = lax.axis_index("probe")
    barrier = pltpu.get_barrier_semaphore()
    paired = n & (n - 1) == 0

    signs = []
    if paired:
        bit = 1
        while bit < n:
            signs.append((1 - 2 * lax.rem(lax.div(me, bit), 2)) * bit)
            bit *= 2

    def code(i):
        return ORDER[i] if n == len(ORDER) else i

    def flip(i):
        out = me
        if isinstance(i, int):
            for b, sign in enumerate(signs):
                if code(i) >> b & 1:
                    out = out + sign
        else:
            for b, sign in enumerate(signs):
                bits = lax.rem(lax.div(i, jnp.int32(1 << b)), 2)
                if n == len(ORDER):
                    bits = sum(jnp.where(i == k, code(k) >> b & 1, 0) for k in range(n))
                out = out + sign * bits
        return out

    def peer_to(i):
        return flip(i) if paired else lax.rem(me + i, n)

    def peer_from(i):
        return flip(i) if paired else lax.rem(me + n - i, n)

    def probe_peer(i):
        return lax.rem(zme + i, z)

    def each(lo, hi, f):
        if hi - lo <= 8:
            for i in range(lo, hi):
                f(i)
        else:
            lax.fori_loop(lo, hi, lambda i, c: (f(i), c)[1], 0)

    def greet(i):
        pl.semaphore_signal(barrier, inc=1, device_id={"surf": peer_to(n - i)}, device_id_type=pl.DeviceIdType.MESH)

    def tell(sem, lo, hi):
        def step(i, c):
            pl.semaphore_signal(sem, inc=1, device_id={"probe": i}, device_id_type=pl.DeviceIdType.MESH)
            return c

        lax.fori_loop(lo, hi, step, 0)

    def settled(ref, sem):
        pltpu.make_async_copy(ref, ref, sem).wait()

    for i, src in enumerate((owner_hbm, slot_hbm)):
        pltpu.make_async_copy(src, index_ref.at[i], load_sem.at[0]).start()
    far = n - 2 if n == len(ORDER) else n
    upper = lax.div(me, 4) if n == len(ORDER) else 1
    each(1, far, lambda i: greet(n - i))
    if far < n:

        @pl.when(upper == 0)
        def _():
            each(far, n, lambda i: greet(n - i))

    tell(barrier, zme + 1, z)

    smalls = ((count_hbm, index_ref.at[2]), (obs_hbm, obs_ref), (patch_hbm, patch_ref), (sigma_hbm, sigma_ref), (probes_hbm, probes_ref))
    loads = [pltpu.make_async_copy(src, dst, load_sem.at[1 + i]) for i, (src, dst) in enumerate(smalls)]
    load_coef = pltpu.make_async_copy(coef_hbm, ext_ref.at[:, pl.ds(0, vol)], load_sem.at[6])
    load_op = pltpu.make_async_copy(op_hbm, op_ref, load_sem.at[7])
    for load in loads + [load_coef, load_op]:
        load.start()
    settled(index_ref.at[0:2], load_sem.at[0])

    square = (blocks, blocks)
    down = lax.broadcasted_iota(jnp.int32, square, 0)
    across = lax.broadcasted_iota(jnp.int32, square, 1)
    owner = jnp.broadcast_to(index_ref[0], square).astype(F32)
    same = (owner == jnp.transpose(owner)) & (down < across)
    rank = jnp.sum(jnp.where(same, 1.0, 0.0), axis=0, keepdims=True)
    key = owner * depth + rank
    turn = lax.div(down, depth)
    if n == len(ORDER):
        slot = turn
        for i in range(n):
            turn = jnp.where(slot == i, code(i), turn)
    if paired:
        turn = jnp.bitwise_xor(turn, me)
    else:
        turn = lax.rem(turn + me, n)
    chosen = key == (turn * depth + lax.rem(down, depth)).astype(F32)
    slots = jnp.broadcast_to(index_ref[1], square).astype(F32)
    asked = jnp.sum(jnp.where(chosen, slots, 0.0), axis=1, keepdims=True)
    asked = jnp.where(across == down, jnp.broadcast_to(asked, square), 0.0).astype(jnp.int32)
    ask_out[...] = jnp.sum(asked.reshape(n, depth, blocks), axis=1, keepdims=True)

    pl.semaphore_wait(barrier, (far - 1) + (n - far) * upper + zme)

    def ask(i, part):
        return pltpu.make_async_remote_copy(
            src_ref=ask_out.at[i],
            dst_ref=ask_in.at[i],
            send_sem=ask_send,
            recv_sem=ask_recv.at[part],
            device_id={"surf": peer_to(i)},
            device_id_type=pl.DeviceIdType.MESH,
        )

    def row(i, part):
        return pltpu.make_async_remote_copy(
            src_ref=row_out.at[i],
            dst_ref=row_in.at[i],
            send_sem=row_send,
            recv_sem=row_recv.at[part],
            device_id={"surf": peer_from(i)},
            device_id_type=pl.DeviceIdType.MESH,
        )

    def quad_copy(i):
        return pltpu.make_async_remote_copy(
            src_ref=quad_in.at[me],
            dst_ref=quad_in.at[me],
            send_sem=quad_send,
            recv_sem=quad_recv,
            device_id={"surf": peer_to(i)},
            device_id_type=pl.DeviceIdType.MESH,
        )

    def diag_copy(i):
        return pltpu.make_async_remote_copy(
            src_ref=diag_in.at[zme],
            dst_ref=diag_in.at[zme],
            send_sem=diag_send,
            recv_sem=diag_recv,
            device_id={"probe": probe_peer(i)},
            device_id_type=pl.DeviceIdType.MESH,
        )

    step = n // PARTS

    def ask_far():
        each(far, n, lambda i: ask(i, i // step).start())

    each(1, far, lambda i: ask(i, i // step if isinstance(i, int) else lax.div(i, step)).start())
    if far < n:

        @pl.when(upper == 1)
        def _():
            ask_far()

        @pl.when((upper == 0) & (lax.rem(me, 2) == 1))
        def _():
            for i in (2, 4):
                pl.semaphore_signal(relay, inc=1, device_id={"surf": peer_to(i)}, device_id_type=pl.DeviceIdType.MESH)

    tell(answer, 0, zme)

    for load in loads[:2]:
        load.wait()
    lane = lax.rem(across, patch)
    block = jnp.sum(jnp.where(chosen, across.astype(F32), 0.0), axis=1, keepdims=True)
    spot = (2 * lax.rem(across, groups) + lax.div(across, groups)).astype(F32)
    place = jnp.where(jnp.broadcast_to(block, square) == spot, 1.0, 0.0)
    gather = place.astype(BF16)
    scatter = jnp.transpose(place).astype(BF16)
    counts = jnp.broadcast_to(index_ref[2], square).astype(F32)
    counts = jnp.sum(jnp.where(chosen, counts, 0.0), axis=1, keepdims=True)
    keep_lane = lax.rem(lax.broadcasted_iota(jnp.int32, (blocks, patch), 1), cols).astype(F32)
    keep = jnp.where(keep_lane < counts, 1.0, 0.0)
    keep_ref[...] = keep
    twice = (
        lax.rem(lax.broadcasted_iota(jnp.int32, (cols, patch), 1), cols)
        == lax.broadcasted_iota(jnp.int32, (cols, patch), 0)
    ).astype(F32).astype(BF16)
    ext_ref[:, vol:] = lax.dot_general(
        obs_ref[...], twice, (((0,), (0,)), ((), ())), preferred_element_type=F32
    ).astype(BF16)

    for load in loads[2:]:
        load.wait()
    values = probes_ref[...].astype(F32)
    stacked = jnp.concatenate([values[:, k * patch:(k + 1) * patch] for k in range(groups)], axis=0)
    value_ref[...] = stacked
    mixed = jnp.dot(stacked.astype(BF16), patch_ref[...], preferred_element_type=F32)
    for k in range(groups):
        spread_ref[k * width:(k + 1) * width, :] = (
            (mixed[k * width:(k + 1) * width] * sigma_ref[k:k + 1, :]).astype(BF16).astype(F32)
        )
    low = lax.broadcasted_iota(jnp.int32, (groups, patch), 1) < cols
    halves = []
    for p in range(width):
        field = spread_ref[pl.ds(p, groups, stride=width), :]
        turned = pltpu.roll(field, cols, 1)
        halves.append(jnp.concatenate([jnp.where(low, field, turned), jnp.where(low, turned, field)], axis=0).astype(BF16))
    ordered = jnp.dot(gather, jnp.concatenate(halves, axis=1), preferred_element_type=F32)
    for p in range(width):
        field_ref[p] = (ordered[:, p * patch:(p + 1) * patch] * keep).astype(BF16)

    load_coef.wait()

    ways = (0, 1 + lax.rem(me, 2), 2 - lax.rem(me, 2), 3)
    extent = step * depth

    def arrived(ref, sem, part):
        if isinstance(part, int):
            if (part + 1) * step > max(part * step, 1):
                settled(ref.at[max(part * step, 1):(part + 1) * step], sem.at[part])
        else:
            settled(ref.at[pl.ds(part * step, step)], sem.at[part])

    def start_of(part):
        return part * extent if isinstance(part, int) else pl.multiple_of(part * extent, extent)

    def serve(part):
        arrived(ask_in, ask_recv, part)
        shape = (extent, blocks)
        wanted = jnp.sum(ask_in[pl.ds(part * step, step)], axis=0)
        if isinstance(part, int) and part == 0:
            wanted = wanted + ask_out[0]
        here = lax.broadcasted_iota(jnp.int32, shape, 1)
        diagonal = here == lax.broadcasted_iota(jnp.int32, shape, 0) + part * extent
        wanted = jnp.sum(jnp.where(diagonal, jnp.broadcast_to(wanted, shape).astype(F32), 0.0), axis=1, keepdims=True)
        pick = jnp.where(jnp.broadcast_to(wanted, shape) == here.astype(F32), 1.0, 0.0).astype(BF16)
        rows = jnp.dot(pick, ext_ref[...], preferred_element_type=F32).astype(BF16)
        row_out[pl.ds(part * step, step)] = rows.reshape(step, depth, rows.shape[1])
        if isinstance(part, int) and part == 0:
            row_in[0] = row_out[0]
            each(1, step, lambda i: row(i, part).start())
        elif isinstance(part, int):
            each(part * step, (part + 1) * step, lambda i: row(i, part).start())
        else:
            each(0, step, lambda i: row(part * step + i, part).start())

    ask_in[0] = jnp.zeros(ask_in.shape[1:], jnp.int32)
    for part in ways:
        serve(part)
        if far < n and isinstance(part, int) and part == 0:

            @pl.when(upper == 0)
            def _():
                pl.semaphore_wait(relay, 1)
                ask_far()

    load_op.wait()

    def column(part):
        got = row_in[pl.ds(part * step, step)].reshape(extent, row_in.shape[2])
        coef = got[:, :vol]
        weight = got[:, vol:].astype(F32)
        lifted = jnp.concatenate(
            [jnp.concatenate([field_ref[p, pl.ds(start_of(part), extent), :]] * tiles, axis=1) * coef for p in range(width)],
            axis=0,
        )
        weight = jnp.concatenate([weight] * tiles, axis=1)
        state = jnp.dot(lifted, op_ref[...], preferred_element_type=F32)
        weighted = jnp.concatenate(
            [(state[p * extent:(p + 1) * extent] * weight).astype(BF16) for p in range(width)], axis=0
        )
        adjoint = lax.dot_general(weighted, op_ref[...], NT, preferred_element_type=F32)
        return adjoint

    def fold(part, adjoint):
        coef = row_in[pl.ds(part * step, step)].reshape(extent, row_in.shape[2])[:, :vol].astype(F32)
        span = pl.ds(start_of(part), extent)
        keep = keep_ref[span, :]
        for p in range(width):
            at = slice(p * extent, (p + 1) * extent)
            total = None
            for t in range(tiles):
                cut = slice(t * patch, (t + 1) * patch)
                term = adjoint[at, cut] * coef[:, cut]
                total = term if total is None else total + term
            total = (total + pltpu.roll(total, cols, 1)) * keep
            sens_ref[span, p * patch:(p + 1) * patch] = total.astype(BF16)

    @pl.when(zme < z - 1)
    def _():
        pl.semaphore_wait(answer, z - 1 - zme)

    before = None
    for part in ways:
        arrived(row_in, row_recv, part)
        if before is not None:
            fold(*before)
        before = part, column(part)
    fold(*before)

    split = jnp.dot(scatter, sens_ref[...], preferred_element_type=F32)
    scaled = []
    for p in range(width):
        cut = slice(p * patch, (p + 1) * patch)
        scaled.append((jnp.where(low, split[:groups, cut], split[groups:, cut]) * sigma_ref[...]).astype(BF16))
    back = lax.dot_general(jnp.concatenate(scaled, axis=0), patch_ref[...], NT, preferred_element_type=F32)
    total = None
    for p in range(width):
        product = value_ref[pl.ds(p, groups, stride=width), :] * back[p * groups:(p + 1) * groups]
        total = product if total is None else total + product
    diag_in[zme] = total.astype(BF16)
    each(1, z, lambda i: diag_copy(i).start())
    energy = []
    for p in range(width):
        term = back[p * groups:(p + 1) * groups]
        value = value_ref[pl.ds(p, groups, stride=width), :]
        energy.append(jnp.sum(value * term, axis=0, keepdims=True))
        hold_ref[pl.ds(p, groups, stride=width), :] = value + term
    quad_in[me] = jnp.concatenate(energy, axis=0)
    each(1, n, lambda i: quad_copy(n - i).start())
    for k in range(groups):
        hess_ref[:, k * patch:(k + 1) * patch] = hold_ref[k * width:(k + 1) * width, :]
    settled(ask_out.at[1:n], ask_send)
    settled(row_out.at[1:n], row_send)
    settled(quad_in.at[1:n], quad_recv)
    energy = lax.fori_loop(1, n, lambda i, s: s + quad_in[i], quad_in[0])
    energy = jnp.broadcast_to(jnp.sum(energy, axis=1, keepdims=True), (width, patch))
    diagonal = lax.broadcasted_iota(jnp.int32, (width, patch), 0) == lax.broadcasted_iota(jnp.int32, (width, patch), 1)
    quad_ref[...] = jnp.sum(jnp.where(diagonal, energy, 0.0), axis=0, keepdims=True)[:, :width]
    settled(quad_in.at[1:n], quad_send)
    settled(diag_in.at[1:z], diag_send)
    settled(diag_in.at[1:z], diag_recv)
    total = diag_in[0].astype(F32)
    for i in range(1, z):
        total = total + diag_in[i].astype(F32)
    diag_ref[...] = total * (1.0 / total_probes)


def settle(hess_in, diag_in, quad_in, hess_out, diag_out, quad_out, sem):
    stops = ((hess_in, hess_out), (diag_in, diag_out), (quad_in, quad_out))
    store = [pltpu.make_async_copy(src, dst, sem.at[i]) for i, (src, dst) in enumerate(stops)]
    for copy in store:
        copy.start()
    for copy in store:
        copy.wait()


def solution(mesh):
    n, z = mesh.shape["surf"], mesh.shape["probe"]

    def body(probes, sigma, prior_patch, owner_map, block_perm, col_counts, coef, obs_weight, column_op):
        width, nodes = probes.shape
        blocks, vol = coef.shape
        patch = prior_patch.shape[0]
        cols = obs_weight.shape[1]
        groups = nodes // patch
        depth = blocks // n
        vmem = pl.BlockSpec(memory_space=pltpu.VMEM)
        hbm = pl.BlockSpec(memory_space=pl.ANY)
        operands = (
            owner_map.reshape(1, blocks),
            block_perm.reshape(1, blocks),
            col_counts.reshape(1, blocks),
            obs_weight.T,
            prior_patch,
            sigma.reshape(groups, patch),
            probes,
            coef,
            column_op,
        )
        results = pl.pallas_call(
            functools.partial(kernel, n, z, width * z),
            out_shape=(
                pltpu.VMEM((width, nodes), F32),
                pltpu.VMEM((groups, patch), F32),
                pltpu.VMEM((1, width), F32),
            ),
            in_specs=[pl.BlockSpec(memory_space=pltpu.HBM)] * 9,
            out_specs=(vmem, vmem, vmem),
            scratch_shapes=[
                pltpu.VMEM((3, 1, blocks), jnp.int32),
                pltpu.VMEM((cols, blocks), BF16),
                pltpu.VMEM((patch, patch), BF16),
                pltpu.VMEM((groups, patch), F32),
                pltpu.VMEM((width, nodes), BF16),
                pltpu.VMEM((vol, vol), BF16),
                pltpu.VMEM((blocks, vol + patch), BF16),
                pltpu.VMEM((n, 1, blocks), jnp.int32),
                pltpu.VMEM((n, 1, blocks), jnp.int32),
                pltpu.VMEM((n, depth, vol + patch), BF16),
                pltpu.VMEM((n, depth, vol + patch), BF16),
                pltpu.VMEM((blocks, patch), F32),
                pltpu.VMEM((groups * width, patch), F32),
                pltpu.VMEM((groups * width, patch), F32),
                pltpu.VMEM((width, blocks, patch), BF16),
                pltpu.VMEM((blocks, width * patch), BF16),
                pltpu.VMEM((groups * width, patch), F32),
                pltpu.VMEM((z, groups, patch), BF16),
                pltpu.VMEM((n, width, patch), F32),
                pltpu.SemaphoreType.DMA((8,)),
                pltpu.SemaphoreType.DMA,
                pltpu.SemaphoreType.DMA((PARTS,)),
                pltpu.SemaphoreType.DMA,
                pltpu.SemaphoreType.DMA((PARTS,)),
                pltpu.SemaphoreType.DMA,
                pltpu.SemaphoreType.DMA,
                pltpu.SemaphoreType.DMA,
                pltpu.SemaphoreType.DMA,
                pltpu.SemaphoreType.REGULAR,
                pltpu.SemaphoreType.REGULAR,
            ],
            compiler_params=pltpu.CompilerParams(
                collective_id=0, has_side_effects=True, vmem_limit_bytes=32 * 1024 * 1024
            ),
        )(*[pltpu.with_memory_space_constraint(x, pltpu.HBM) for x in operands])
        hess, diag, quad = pl.pallas_call(
            settle,
            out_shape=tuple(jax.ShapeDtypeStruct(r.shape, r.dtype) for r in results),
            in_specs=[vmem] * 3,
            out_specs=(hbm,) * 3,
            scratch_shapes=[pltpu.SemaphoreType.DMA((3,))],
            compiler_params=pltpu.CompilerParams(vmem_limit_bytes=1024 * 1024),
        )(*results)
        return hess, diag.reshape(nodes), quad.reshape(width)

    in_specs = (
        P("probe", "surf"),
        P("surf"),
        P(),
        P("surf"),
        P("surf"),
        P("surf"),
        P("surf", None),
        P("surf", None),
        P(),
    )
    out_specs = (P("probe", "surf"), P("surf"), P("probe"))
    return jax.shard_map(body, mesh=mesh, in_specs=in_specs, out_specs=out_specs, check_vma=False)
```
